128 devices in a mesh: dp: 8 (over z, y_lo), tensor: 16 (over x, y_hi, core).
Axes of the slice: x: 4, y: 4 (y_hi: 2, y_lo: 2; y = y_hi * 2 + y_lo), z: 4, core: 2. Of those that a mesh axis runs over, the one named last changes fastest.
Arguments:
- projected: bfloat16 [2, 16384, 4608], P(None, ('dp', 'tensor')), may hold values from -60 to 60
- out_grad: bfloat16 [2, 16384, 4608], P(None, ('dp', 'tensor')), may hold values from -20 to 20
- attention: bfloat16 [2, 16384, 4096], P(None, 'dp', 'tensor'), may hold values from -6 to 6
- w_out: bfloat16 [4096, 4608], P('tensor'), may hold values from -0.09375 to 0.09375
- gains: float32 [4608], replicated, may hold values from 0.5 to 1.5
- main_out: float32 [4096, 4608], P('tensor', 'dp'), may hold values from -6 to 6
- main_gains: float32 [4608], replicated, may hold values from -6 to 6
Outputs:
- attn_grad: bfloat16 [2, 16384, 4096], P(None, 'dp', 'tensor')
- new_main_out: float32 [4096, 4608], P('tensor', 'dp')
- new_main_gains: float32 [4608], replicated
The draws below stay inside these ranges and needn't reach their ends.
All inputs are finite; a program needn't handle non-finite values.
Results may differ from the reference program's by a relative error of at most 0.0049.
Values may be sent and summed in bfloat16 or wider, within the bound.
No kernel may reach another device: no remote copies, remote signals or barrier semaphores. Data moves between devices by JAX's collectives and lax.ppermute only.
A program may use at most 128 MiB of HBM per device.

```python
import math
import jax
import jax.numpy as jnp
from jax import lax

D = 4608
HQ = 4096
MICRO = 2
ROWS = 16384


def spread_values(key, shape):
    first, second, third = jax.random.split(key, 3)
    base = jnp.clip(jax.random.normal(first, shape), -6.0, 6.0)
    columns = jnp.exp(jax.random.uniform(second, (shape[-1],), minval=math.log(0.3), maxval=math.log(3.0)))
    row_scale = jnp.exp(jax.random.uniform(third, shape[:-1] + (1,), minval=math.log(0.3), maxval=math.log(3.0)))
    return base * row_scale * columns


def rising_values(key, shape):
    position = jnp.arange(shape[1], dtype=jnp.float32) / shape[1]
    base = jnp.clip(jax.random.normal(key, shape), -6.0, 6.0)
    growth = jnp.exp(position * math.log(3.0))
    return base * growth[None, :, None]


def draw_projected(key, part):
    return spread_values(jax.random.fold_in(key, 22), (MICRO, ROWS, D)).astype(jnp.bfloat16)


def draw_out_grad(key, part):
    return rising_values(jax.random.fold_in(key, 33), (MICRO, ROWS, D)).astype(jnp.bfloat16)


def steps_of(stream_key, dims, cuts, low, high):
    def one(axis_at, shards_of):
        steps = jax.random.uniform(jax.random.fold_in(jax.random.fold_in(stream_key, 6), axis_at), (shards_of,), jnp.float32, low / len(cuts), high / len(cuts))
        return jnp.repeat(jnp.exp(steps), dims[axis_at] // shards_of).reshape((-1,) + (1,) * (len(dims) - axis_at - 1))

    loudness = one(*cuts[0])
    for cut in cuts[1:]:
        loudness = loudness * one(*cut)
    return loudness


def scatter_about(own_key, dims, spread, reach, cuts=(), held_as=jnp.bfloat16):
    result = jax.random.normal(own_key, dims, jnp.float32) * spread
    if len(cuts) > 0:
        result = steps_of(own_key, dims, cuts, -0.22, 0.18) * result
    return jnp.clip(result, min=-reach, max=reach).astype(held_as)


def setup_inputs(seed: int = 0) -> dict:
    keys = jax.random.split(jax.random.key(seed), 8)
    return {
        "projected": draw_projected(jax.random.fold_in(keys[7], 71), 0),
        "out_grad": draw_out_grad(jax.random.fold_in(keys[7], 71), 0),
        "attention": scatter_about(keys[2], (MICRO, ROWS, HQ), 1.0, 6.0, ((1, 8), (2, 16))),
        "w_out": scatter_about(keys[3], (HQ, D), HQ ** -0.5, 0.09375, ((0, 16),)),
        "gains": jnp.clip(1.0 + 0.1 * jax.random.normal(keys[4], (D,), jnp.float32), 0.5, 1.5),
        "main_out": scatter_about(keys[5], (HQ, D), 1.0, 6.0, ((0, 16), (1, 8)), jnp.float32),
        "main_gains": scatter_about(keys[6], (D,), 1.0, 6.0, (), jnp.float32),
    }


def normalized(values):
    inverse = lax.rsqrt(lax.optimization_barrier(jnp.mean(values * values, axis=-1, keepdims=True)) + 1e-06)
    return (values * inverse, inverse)

def norm_back(upstream, normed, inverse):
    return inverse * (upstream - normed * lax.optimization_barrier(jnp.mean(upstream * normed, axis=-1, keepdims=True)))

def reference(projected, out_grad, attention, w_out, gains, main_out, main_gains):
    factor = 1.0 / (MICRO * ROWS) ** 0.5
    sum_out = jnp.zeros((HQ, D), jnp.float32)
    sum_gain = jnp.zeros((D,), jnp.float32)
    attn_list = []
    for micro_step in range(MICRO):
        output_in = projected[micro_step].astype(jnp.float32)
        upstream = out_grad[micro_step].astype(jnp.float32)
        out_hat, out_inv = normalized(output_in)
        out_gain = lax.optimization_barrier(jnp.sum(upstream * out_hat, axis=0))
        out_back = norm_back(upstream * gains, out_hat, out_inv).astype(jnp.bfloat16)
        attn_list.append(jnp.dot(out_back, w_out.T, preferred_element_type=jnp.float32).astype(jnp.bfloat16))
        sum_out = sum_out + jnp.dot(attention[micro_step].T, out_back, preferred_element_type=jnp.float32)
        sum_gain = sum_gain + out_gain
    return (jnp.stack(attn_list), main_out + factor * sum_out, main_gains + factor * sum_gain)
```

```python
import functools
import math

import jax
import jax.numpy as jnp
from jax import lax
from jax.experimental import pallas as pl
from jax.experimental.pallas import tpu as pltpu
from jax.sharding import Mesh
from jax.sharding import PartitionSpec as P

Z, YL, X, YH, C = AXES = ("dp_0", "dp_1", "tensor_0", "tensor_1", "tensor_2")
DP = (Z, YL)
TENSOR = (X, YH, C)
BF16 = jnp.bfloat16
F32 = jnp.float32

PIECES = ((0, 512), (512, 384), (896, 256))
RELATIVE = (0, -1, 1, 2)


def ring(step, size=4):
    return [(i, (i + step) % size) for i in range(size)]


def swap(size=2):
    return [(i, size - 1 - i) for i in range(size)]


def params(semantics, mib=56):
    return pltpu.CompilerParams(dimension_semantics=semantics, vmem_limit_bytes=mib * 1024 * 1024)


def nt(lhs, rhs):
    return lax.dot_general(lhs, rhs, (((1,), (1,)), ((), ())), preferred_element_type=F32)


def norm_kernel(width, values, upstream, gains, *outs):
    pieces, total = outs[:-1], outs[-1]
    v = values[0].astype(F32)
    u = upstream[0].astype(F32)
    inverse = lax.rsqrt(jnp.mean(v * v, axis=-1, keepdims=True) + 1e-06)
    n = v * inverse
    gain = jnp.sum((u * n).reshape(-1, 8, u.shape[-1]), axis=0)

    @pl.when((pl.program_id(0) == 0) & (pl.program_id(1) == 0))
    def _():
        total[...] = jnp.zeros_like(total)

    total[...] += gain
    w = u * gains[...]
    back = (inverse * (w - n * jnp.mean(w * n, axis=-1, keepdims=True))).astype(BF16)
    for (start, size), out in zip(PIECES, pieces):
        for z in range(4):
            out[0, :, z * size : (z + 1) * size] = back[:, z * width + start : z * width + start + size]


def norm_pieces(projected, out_grad, gains):
    micro, rows, cols = projected.shape
    step = 32
    block = pl.BlockSpec((1, step, cols), lambda m, i: (m, i, 0))
    return pl.pallas_call(
        functools.partial(norm_kernel, cols // 4),
        grid=(micro, rows // step),
        in_specs=[block, block, pl.BlockSpec((1, cols), lambda m, i: (0, 0))],
        out_specs=[pl.BlockSpec((1, step, 4 * s), lambda m, i: (m, i, 0)) for _, s in PIECES]
        + [pl.BlockSpec((8, cols), lambda m, i: (0, 0))],
        out_shape=[jax.ShapeDtypeStruct((micro, rows, 4 * s), BF16) for _, s in PIECES]
        + [jax.ShapeDtypeStruct((8, cols), F32)],
        compiler_params=params(("arbitrary", "arbitrary")),
        cost_estimate=pl.CostEstimate(
            flops=16 * micro * rows * cols, bytes_accessed=6 * micro * rows * cols, transcendentals=0
        ),
        name="norm_back",
    )(projected, out_grad, gains.reshape(1, cols))


def turn_kernel(place, *refs):
    out = refs[-1]
    for i, ref in enumerate(refs[:-1]):
        out[:, i * 128 : (i + 1) * 128] = ref[0, 0].T


def turned(attention, place, across, other):
    micro, rows, heads = attention.shape
    blocks = attention.reshape(micro, 16, rows // 16, heads)

    def spec(j, m):
        def index(i, p):
            return (m, lax.rem(p[0] + RELATIVE[j] + 4, 4) * 4 + (p[1] ^ across) * 2 + (p[2] ^ other), 0, 0)

        return pl.BlockSpec((1, 1, rows // 16, heads), index)

    specs = [spec(j, m) for j in range(4) for m in range(micro)]
    return pl.pallas_call(
        turn_kernel,
        grid_spec=pltpu.PrefetchScalarGridSpec(
            num_scalar_prefetch=1,
            grid=(1,),
            in_specs=specs,
            out_specs=pl.BlockSpec((heads, len(specs) * 128), lambda i, p: (0, 0)),
        ),
        out_shape=jax.ShapeDtypeStruct((heads, len(specs) * 128), BF16),
        compiler_params=params(("arbitrary",)),
        cost_estimate=pl.CostEstimate(flops=1000000, bytes_accessed=4 * heads * 1024, transcendentals=0),
        name="turn",
    )(place, *([blocks] * len(specs)))


def data_kernel(groups, width, *refs):
    n = len(PIECES)
    rows = refs[: groups * n]
    weights = refs[groups * n : groups * n + 4]
    outs = refs[groups * n + 4 : groups * n + 8]
    acc = refs[-1]
    z = pl.program_id(0)

    @pl.when(z == 0)
    def _():
        acc[...] = jnp.zeros_like(acc)

    lhs = jnp.concatenate(
        [
            jnp.concatenate([rows[g * n + k][...].reshape(256, -1) for k in range(n)], axis=1)
            for g in range(groups)
        ],
        axis=0,
    )
    for h in range(4):
        acc[h] += nt(lhs, weights[h][...])

    @pl.when(z == 3)
    def _():
        for h in range(4):
            outs[h][...] = acc[h].astype(BF16).reshape(outs[h].shape)


def data_grad(groups, weights):
    count = len(groups)
    width = weights[0].shape[1] // 4
    flat = [piece for group in groups for piece in group]
    shape = (count, 2, 128, 256)
    return pl.pallas_call(
        functools.partial(data_kernel, count, width),
        grid=(4,),
        in_specs=[pl.BlockSpec((2, 128, p.shape[2] // 4), lambda z: (0, 0, z)) for p in flat]
        + [pl.BlockSpec((256, width), lambda z: (0, z)) for _ in weights],
        out_specs=[pl.BlockSpec(shape, lambda z: (0, 0, 0, 0))] * 4,
        out_shape=[jax.ShapeDtypeStruct(shape, BF16)] * 4,
        scratch_shapes=[pltpu.VMEM((4, 256 * count, 256), F32)],
        compiler_params=params(("arbitrary",)),
        cost_estimate=pl.CostEstimate(
            flops=2 * 256 * count * 1024 * 4 * width, bytes_accessed=8 * 1024 * width, transcendentals=0
        ),
        name="data_grad",
    )(*flat, *weights)


def sum_kernel(own, left, right, far_a, far_b, *refs):
    heads, keep, send = refs[:4], refs[4], refs[5]
    size = own.shape[-1]
    rows = jnp.concatenate(
        [r[...].reshape(256, size) for r in (own, left, right)] + [far_a[...], far_b[...]], axis=0
    )
    for i, h in enumerate(heads):
        out = jnp.dot(h[...], rows, preferred_element_type=F32).astype(BF16)
        (keep, send)[i // 2][0, i % 2] = out


def weight_sum(own, left, right, far_a, far_b, heads):
    size = own.shape[2] // 4
    wide = pl.BlockSpec((2, 128, size), lambda z: (0, 0, z))
    half = pl.BlockSpec((128, size), lambda z: (0, z))
    out = pl.BlockSpec((1, 2, 256, size), lambda z: (z, 0, 0, 0))
    return pl.pallas_call(
        sum_kernel,
        grid=(4,),
        in_specs=[wide] * 3 + [half] * 2 + [pl.BlockSpec((256, 1024), lambda z: (0, 0))] * 4,
        out_specs=[out] * 2,
        out_shape=[jax.ShapeDtypeStruct((4, 2, 256, size), BF16)] * 2,
        compiler_params=params(("arbitrary",)),
        cost_estimate=pl.CostEstimate(
            flops=8 * 1024 * 1024 * size, bytes_accessed=20 * 1024 * size, transcendentals=0
        ),
        name="weight_sum",
    )(own, left, right, far_a, far_b, *heads)


def place_kernel(place, a, b, c, d, *refs):
    out = refs[-1]
    for i, ref in enumerate((a, b, c, d)):

        @pl.when(pl.program_id(1) == i)
        def _():
            out[...] = ref[0][:, None]


def placed(place, blocks, first, into=None):
    count = blocks[0].shape[0]
    shape = (2, 16, 128, 256)

    def index(j, i, p):
        rel = jnp.int32(RELATIVE[first])
        for t in range(1, count):
            rel = jnp.where(j == t, RELATIVE[first + t], rel)
        return (0, lax.rem(p[0] + rel + 4, 4) * 4 + (p[1] ^ (i // 2)) * 2 + (p[2] ^ lax.rem(i, 2)), 0, 0)

    ins = [pl.BlockSpec((1, 2, 128, 256), lambda j, i, p: (j, 0, 0, 0))] * 4
    args = [place, *blocks]
    if into is not None:
        ins.append(pl.BlockSpec(memory_space=pl.ANY))
        args.append(into)
    return pl.pallas_call(
        place_kernel,
        grid_spec=pltpu.PrefetchScalarGridSpec(
            num_scalar_prefetch=1,
            grid=(count, 4),
            in_specs=ins,
            out_specs=pl.BlockSpec((2, 1, 128, 256), index),
        ),
        out_shape=jax.ShapeDtypeStruct(shape, BF16),
        input_output_aliases={} if into is None else {5: 0},
        compiler_params=params(("arbitrary", "arbitrary")),
        cost_estimate=pl.CostEstimate(
            flops=1000000, bytes_accessed=count * 8 * 128 * 256 * 4, transcendentals=0
        ),
        name="place",
    )(*args)


def per_device(projected, out_grad, attention, w_out, gains, main_out, main_gains):
    micro, own_rows, cols = projected.shape
    tokens_all = micro * own_rows * lax.axis_size(AXES)
    factor = 1.0 / math.sqrt(tokens_all)
    place = jnp.stack([lax.axis_index(X), lax.axis_index(YH), lax.axis_index(C)])
    here = lax.axis_index(Z)
    low = lax.axis_index(YL)
    both = (YL, YH)

    *own, gain = norm_pieces(projected, out_grad, gains)
    left = [lax.ppermute(p, X, ring(1)) for p in own]
    right = [lax.ppermute(p, X, ring(-1)) for p in own]
    far_a = [lax.ppermute(p[0], X, ring(1)) for p in left]
    far_b = [lax.ppermute(p[1], X, ring(-1)) for p in right]

    mine = turned(attention, place, 0, 0)
    mate = lax.ppermute(turned(attention, place, 0, 1), C, swap())
    over = lax.ppermute(turned(attention, place, 1, 0), YH, swap())
    over_mate = lax.ppermute(lax.ppermute(turned(attention, place, 1, 1), YH, swap()), C, swap())
    heads = (mine, over, mate, over_mate)

    w_over = lax.ppermute(w_out, both, swap(4))
    w_mate = lax.ppermute(w_out, C, swap())
    w_over_mate = lax.ppermute(w_over, C, swap())
    weights = (w_out, w_mate, w_over, w_over_mate)

    gain = jnp.sum(gain, axis=0)
    for axis, perm in (
        (X, [(i, i ^ 1) for i in range(4)]),
        (X, [(i, i ^ 2) for i in range(4)]),
        (Z, [(i, i ^ 1) for i in range(4)]),
        (Z, [(i, i ^ 2) for i in range(4)]),
        (YL, swap()),
        (YH, swap()),
        (C, swap()),
    ):
        gain = gain + lax.ppermute(gain, axis, perm)
    new_gains = main_gains + factor * gain

    def exchanged(outs):
        o00, o01, o10, o11 = outs
        r0 = lax.ppermute(o10, YH, swap())
        r1 = lax.ppermute(o11, YH, swap())
        return (o00, lax.ppermute(o01, C, swap()), r0, lax.ppermute(r1, C, swap()))

    near = data_grad([own, left, right], weights)
    near = exchanged(near)
    grad = placed(place, near, 0)

    def reduced(k):
        keep, send = weight_sum(own[k], left[k], right[k], far_a[k], far_b[k], heads)
        other = lax.ppermute(send, C, swap())

        def part(step):
            at = lax.rem(here + step + 4, 4)
            a = lax.dynamic_index_in_dim(keep, at, 0, keepdims=False).astype(F32)
            b = lax.dynamic_index_in_dim(other, at, 0, keepdims=False).astype(F32)
            return a + b

        total = part(0)
        for step in (1, -1, 2):
            total = total + lax.ppermute(part(step).astype(BF16), Z, ring(step)).astype(F32)
        return total.astype(BF16)

    parts = [reduced(k) for k in range(len(PIECES))]
    far = [
        jnp.stack([a, b]) for a, b in zip(far_a, far_b)
    ]
    far_out = exchanged(data_grad([far], weights))
    grad = placed(place, far_out, 3, grad)

    whole = jnp.concatenate(parts, axis=2)
    halves = jnp.where(low == 0, whole[:, :, : cols // 8], whole[:, :, cols // 8 :])
    others = jnp.where(low == 0, whole[:, :, cols // 8 :], whole[:, :, : cols // 8])
    total = halves[0].astype(F32)
    total = total + lax.ppermute(others[0], YL, swap()).astype(F32)
    total = total + lax.ppermute(halves[1], YH, swap()).astype(F32)
    total = total + lax.ppermute(others[1], both, swap(4)).astype(F32)
    return (grad.reshape(attention.shape), main_out + factor * total, new_gains)


def solution(mesh):
    torus = Mesh(mesh.devices.reshape(4, 2, 4, 2, 2), AXES)
    return jax.shard_map(
        per_device,
        mesh=torus,
        in_specs=(
            P(None, AXES, None),
            P(None, AXES, None),
            P(None, DP, TENSOR),
            P(TENSOR, None),
            P(),
            P(TENSOR, DP),
            P(),
        ),
        out_specs=(P(None, DP, TENSOR), P(TENSOR, DP), P()),
        check_vma=False,
    )
```

```python
import functools
import math

import jax
import jax.numpy as jnp
from jax import lax
from jax.experimental import pallas as pl
from jax.experimental.pallas import tpu as pltpu
from jax.sharding import Mesh
from jax.sharding import PartitionSpec as P

Z, YL, X, YH, C = AXES = ("dp_0", "dp_1", "tensor_0", "tensor_1", "tensor_2")
DP = (Z, YL)
TENSOR = (X, YH, C)
BF16 = jnp.bfloat16
F32 = jnp.float32

PIECES = (((0, 512),), ((512, 384),), ((896, 256),))
SIZES = tuple(sum(size for _, size in runs) for runs in PIECES)
SUMS = ((0,), (1, 2))
RELATIVE = (0, -1, 1, 2)


def ring(step, size=4):
    return [(i, (i + step) % size) for i in range(size)]


def swap(size=2):
    return [(i, size - 1 - i) for i in range(size)]


def params(semantics, mib=56):
    return pltpu.CompilerParams(dimension_semantics=semantics, vmem_limit_bytes=mib * 1024 * 1024)


def cost(flops, moved):
    return pl.CostEstimate(flops=flops, bytes_accessed=moved, transcendentals=0)


def nt(lhs, rhs):
    return lax.dot_general(lhs, rhs, (((1,), (1,)), ((), ())), preferred_element_type=F32)


def near(position, j):
    if not isinstance(j, int):
        offset = jnp.where(j == 1, 3, jnp.where(j == 2, 1, jnp.where(j == 3, 2, 0)))
    else:
        offset = RELATIVE[j] % 4
    return lax.rem(position + offset, 4)


def norm_kernel(width, values, upstream, gains, *outs):
    pieces, total = outs[:-1], outs[-1]
    v = values[0].astype(F32)
    u = upstream[0].astype(F32)
    inverse = lax.rsqrt(jnp.mean(v * v, axis=-1, keepdims=True) + 1e-06)
    n = v * inverse
    gain = jnp.sum((u * n).reshape(-1, 8, u.shape[-1]), axis=0)

    @pl.when((pl.program_id(0) == 0) & (pl.program_id(1) == 0))
    def _():
        total[...] = jnp.zeros_like(total)

    total[...] += gain
    w = u * gains[...][None, :]
    back = (inverse * (w - n * jnp.mean(w * n, axis=-1, keepdims=True))).astype(BF16)
    for runs, out in zip(PIECES, pieces):
        at = 0
        for z in range(4):
            for start, size in runs:
                out[0, :, at : at + size] = back[:, z * width + start : z * width + start + size]
                at += size


def norm_pieces(projected, out_grad, gains, step=64):
    micro, rows, cols = projected.shape
    block = pl.BlockSpec((1, step, cols), lambda m, i: (m, i, 0))
    return pl.pallas_call(
        functools.partial(norm_kernel, cols // 4),
        grid=(micro, rows // step),
        in_specs=[block, block, pl.BlockSpec((cols,), lambda m, i: (0,))],
        out_specs=[pl.BlockSpec((1, step, 4 * s), lambda m, i: (m, i, 0)) for s in SIZES]
        + [pl.BlockSpec((8, cols), lambda m, i: (0, 0))],
        out_shape=[jax.ShapeDtypeStruct((micro, rows, 4 * s), BF16) for s in SIZES]
        + [jax.ShapeDtypeStruct((8, cols), F32)],
        compiler_params=params(("arbitrary", "arbitrary")),
        cost_estimate=cost(16 * micro * rows * cols, 6 * micro * rows * cols),
        name="norm_back",
    )(projected, out_grad, gains)


def turn_kernel(place, eye, *refs):
    mine, over = refs[-2:]
    rows = jnp.concatenate([r[0, 0] for r in refs[:-2]], axis=0)
    part = nt(eye[...], rows).astype(BF16)

    @pl.when(pl.program_id(0) < 2)
    def _():
        over[0] = part

    @pl.when(pl.program_id(0) >= 2)
    def _():
        mine[0] = part


def turned(attention, place):
    micro, rows, heads = attention.shape
    each = rows // 16
    blocks = attention.reshape(micro, 16, each, heads)

    def spec(j, m):
        def index(i, p):
            return (m, near(p[0], j) * 4 + (p[1] ^ 1 ^ (i // 2)) * 2 + (p[2] ^ (i % 2)), 0, 0)

        return pl.BlockSpec((1, 1, each, heads), index)

    specs = [spec(j, m) for j in range(4) for m in range(micro)]
    shape = (2, heads, 4 * micro * each)
    block = (1,) + shape[1:]
    return pl.pallas_call(
        turn_kernel,
        grid_spec=pltpu.PrefetchScalarGridSpec(
            num_scalar_prefetch=1,
            grid=(4,),
            in_specs=[pl.BlockSpec((heads, heads), lambda i, p: (0, 0))] + specs,
            out_specs=[
                pl.BlockSpec(block, lambda i, p: (jnp.maximum(i - 2, 0), 0, 0)),
                pl.BlockSpec(block, lambda i, p: (jnp.minimum(i, 1), 0, 0)),
            ],
        ),
        out_shape=[jax.ShapeDtypeStruct(shape, BF16)] * 2,
        compiler_params=params(("arbitrary",)),
        cost_estimate=cost(8 * heads * heads * shape[2], 16 * heads * shape[2]),
        name="turn",
    )(place, jnp.eye(heads, dtype=BF16), *([blocks] * len(specs)))


def data_kernel(plan, carried, last, place, *refs):
    del place
    acc, refs = refs[-1], list(refs[:-1])
    step = pl.program_id(0)
    sides = []
    for pieces, number in plan:
        parts = []
        for _ in pieces:
            take, refs = refs[:number], refs[number:]
            parts.append(jnp.concatenate([r[...].reshape(-1, r.shape[-1]) for r in take], axis=0))
        sides.append(parts[0] if len(parts) == 1 else jnp.concatenate(parts, axis=1))
    weights, refs = refs[:4], refs[4:]
    before = refs.pop(0) if carried else None

    @pl.when(step == 0)
    def _():
        acc[...] = jnp.zeros_like(acc)
        if carried:
            acc[:, : before.shape[1]] = before[...]

    for h, w in enumerate(weights):
        at = 0
        for (pieces, _), lhs in zip(plan, sides):
            start = PIECES[pieces[0]][0][0]
            columns = slice(start, start + lhs.shape[1])
            acc[h, at : at + lhs.shape[0]] += nt(lhs, w[:, columns])
            at += lhs.shape[0]

    @pl.when(step == 3)
    def _():
        for h in range(4):
            if last:
                out = refs[h // 2]
                out[h % 2] = acc[h].astype(BF16).reshape(out.shape[1:])
            else:
                refs[0][h] = acc[h]


def data_grad(place, plan, weights, before=None, last=True):
    flat = [a for _, arrays in plan for piece in arrays for a in piece]
    width = weights[0].shape[1] // 4
    rows = sum(sum(math.prod(a.shape[:-1]) for a in arrays[0]) for _, arrays in plan)

    def rows_spec(a):
        size = a.shape[-1] // 4
        if len(a.shape) == 3:
            return pl.BlockSpec(a.shape[:2] + (size,), lambda t, p: (0, 0, t))
        return pl.BlockSpec((a.shape[0], size), lambda t, p: (0, t))

    held = pl.BlockSpec((4, rows if before is None else before.shape[1], 256), lambda t, p: (0, 0, 0))
    shape = (2, rows // 256, 2, 128, 256)
    args = [*flat, *weights]
    specs = [rows_spec(a) for a in flat] + [pl.BlockSpec((256, width), lambda t, p: (0, t))] * 4
    if before is not None:
        args.append(before)
        specs.append(held)
    flops = sum(
        2 * math.prod(a.shape) * 1024 for _, arrays in plan for piece in arrays for a in piece
    )
    return pl.pallas_call(
        functools.partial(
            data_kernel, [(k, len(a[0])) for k, a in plan], before is not None, last
        ),
        grid_spec=pltpu.PrefetchScalarGridSpec(
            num_scalar_prefetch=1,
            grid=(4,),
            in_specs=specs,
            out_specs=[pl.BlockSpec(shape, lambda t, p: (0, 0, 0, 0, 0))] * 2 if last else held,
            scratch_shapes=[pltpu.VMEM((4, rows, 256), F32)],
        ),
        out_shape=[jax.ShapeDtypeStruct(shape, BF16)] * 2
        if last
        else jax.ShapeDtypeStruct((4, rows, 256), F32),
        compiler_params=params(("arbitrary",)),
        cost_estimate=cost(flops, 8 * 1024 * width),
        name="data_grad",
    )(place, *args)


def weight_sum(pieces, heads):
    sizes = [piece[0].shape[2] // 4 for piece in pieces]
    total = sum(sizes)
    zs = 1 if total % 512 == 0 else 2
    out = pl.BlockSpec((zs, 2, 256, total), lambda i: (i, 0, 0, 0))
    one = pl.BlockSpec((1, 256, 1024), lambda i: (0, 0, 0))
    two = pl.BlockSpec((2, 256, 1024), lambda i: (0, 0, 0))
    specs = []
    for size in sizes:
        specs += [pl.BlockSpec((2, 128, zs * size), lambda i: (0, 0, i))] * 3
        specs += [pl.BlockSpec((128, zs * size), lambda i: (0, i))] * 2
    mine, over, mates = heads

    def kernel(*refs):
        mine, over, mates, keep, send = refs[-5:]
        at = 0
        for k, size in enumerate(sizes):
            rows = jnp.concatenate(
                [r[...].reshape(-1, zs * size) for r in refs[5 * k : 5 * k + 5]], axis=0
            )
            for to, h, block in (
                (keep, 0, mine[0]),
                (keep, 1, over[0]),
                (send, 0, mates[0]),
                (send, 1, mates[1]),
            ):
                part = jnp.dot(block, rows, preferred_element_type=F32).astype(BF16)
                for n in range(zs):
                    to[n, h, :, at : at + size] = part[:, n * size : (n + 1) * size]
            at += size

    return pl.pallas_call(
        kernel,
        grid=(4 // zs,),
        in_specs=specs + [one, one, two],
        out_specs=[out] * 2,
        out_shape=[jax.ShapeDtypeStruct((4, 2, 256, total), BF16)] * 2,
        compiler_params=params(("arbitrary",)),
        cost_estimate=cost(8 * 1024 * 1024 * total, 20 * 1024 * total),
        name="weight_sum",
    )(*[a for piece in pieces for a in piece], mine, over, mates)


def place_kernel(place, mine, over, mates, out):
    for j in range(4):
        for h, block in enumerate((mine.at[0], mates.at[0], over.at[0], mates.at[1])):
            at = near(place[0], j) * 4 + (place[1] ^ (h // 2)) * 2 + (place[2] ^ (h % 2))
            out[:, pl.ds(at, 1)] = block[j][:, None]


def placed(place, blocks):
    mine, over, mates = blocks
    shape = mine.shape[1:]
    one = pl.BlockSpec((1,) + shape, lambda i, p: (0, 0, 0, 0, 0))
    two = pl.BlockSpec((2,) + shape, lambda i, p: (0, 0, 0, 0, 0))
    return pl.pallas_call(
        place_kernel,
        grid_spec=pltpu.PrefetchScalarGridSpec(
            num_scalar_prefetch=1,
            grid=(1,),
            in_specs=[one, one, two],
            out_specs=pl.BlockSpec((2, 16, 128, 256), lambda i, p: (0, 0, 0, 0)),
        ),
        out_shape=jax.ShapeDtypeStruct((2, 16, 128, 256), BF16),
        compiler_params=params(("arbitrary",)),
        cost_estimate=cost(1000000, 16 * 1024 * 1024 // 2),
        name="place",
    )(place, mine, over, mates)


def moved(value, axis, pairs):
    return lax.ppermute(value, axis, pairs)


def per_device(projected, out_grad, attention, w_out, gains, main_out, main_gains):
    micro, own_rows, cols = projected.shape
    tokens_all = micro * own_rows * lax.axis_size(AXES)
    factor = 1.0 / math.sqrt(tokens_all)
    here, low = lax.axis_index(Z), lax.axis_index(YL)
    place = jnp.stack([lax.axis_index(X), lax.axis_index(YH), lax.axis_index(C)])

    *own, gain = norm_pieces(projected, out_grad, gains)
    left = [moved(p, X, ring(1)) for p in own]
    right = [moved(p, X, ring(-1)) for p in own]
    far = []
    for k in range(len(own)):
        a, b = left[k][0], right[k][1]
        far.append((moved(a, X, ring(1)), moved(b, X, ring(-1))))

    def exchanged(mine, over):
        over = moved(over, YH, swap())
        mates = jnp.stack([mine[1], over[1]])
        return mine, over, moved(mates, C, swap())

    heads = exchanged(*turned(attention, place))

    over = moved(w_out, (YL, YH), swap(4))
    weights = (w_out, moved(w_out, C, swap()), over, moved(over, C, swap()))

    gain = jnp.sum(gain, axis=0)
    for axis, bit in ((YH, 1), (YL, 1), (Z, 1), (Z, 2), (C, 1), (X, 1), (X, 2)):
        pairs = [(i, i ^ bit) for i in range(lax.axis_size(axis))]
        gain = gain + moved(gain, axis, pairs)
    new_gains = main_gains + factor * gain

    plan = [
        (tuple(range(len(own))), [(own[k], left[k], right[k]) for k in range(len(own))]),
        (tuple(range(len(own))), far),
    ]
    outs = data_grad(place, plan, weights)
    grad = placed(place, exchanged(*outs))

    def reduced(k):
        pieces = [(own[i], left[i], right[i], *far[i]) for i in SUMS[k]]
        keep, send = weight_sum(pieces, heads)
        other = moved(send, C, swap())

        def block(step):
            at = lax.rem(here + step + 4, 4)
            a = lax.dynamic_index_in_dim(keep, at, 0, keepdims=False).astype(F32)
            return a + lax.dynamic_index_in_dim(other, at, 0, keepdims=False).astype(F32)

        got = [moved(block(step).astype(BF16), Z, ring(step)) for step in (1, -1, 2)]
        return (block(0) + sum(g.astype(F32) for g in got)).astype(BF16)

    whole = jnp.concatenate([reduced(k) for k in range(len(SUMS))], axis=2)
    first, second = whole[:, :, : cols // 8], whole[:, :, cols // 8 :]
    ours, theirs = jnp.where(low == 0, first, second), jnp.where(low == 0, second, first)
    total = ours[0].astype(F32)
    for value, axes, pairs in ((theirs[0], YL, swap()), (ours[1], YH, swap()), (theirs[1], (YL, YH), swap(4))):
        total += moved(value, axes, pairs).astype(F32)
    return (grad.reshape(attention.shape), main_out + factor * total, new_gains)


def solution(mesh):
    torus = Mesh(mesh.devices.reshape(4, 2, 4, 2, 2), AXES)

    return jax.shard_map(
        per_device,
        mesh=torus,
        in_specs=(
            P(None, AXES, None),
            P(None, AXES, None),
            P(None, DP, TENSOR),
            P(TENSOR, None),
            P(),
            P(TENSOR, DP),
            P(),
        ),
        out_specs=(P(None, DP, TENSOR), P(TENSOR, DP), P()),
        check_vma=False,
    )
```

```python
import functools
import math

import jax
import jax.numpy as jnp
from jax import lax
from jax.experimental import pallas as pl
from jax.experimental.pallas import tpu as pltpu
from jax.sharding import Mesh
from jax.sharding import PartitionSpec as P

Z, YL, X, YH, C = AXES = ("dp_0", "dp_1", "tensor_0", "tensor_1", "tensor_2")
DP = (Z, YL)
TENSOR = (X, YH, C)
BF16 = jnp.bfloat16
F32 = jnp.float32

PIECES = (((0, 256),), ((256, 512),), ((768, 384),))
SIZES = tuple(sum(size for _, size in runs) for runs in PIECES)
SUMS = ((0,), (1,), (2,))
RELATIVE = (0, -1, 1, 2)


def ring(step, size=4):
    return [(i, (i + step) % size) for i in range(size)]


def swap(size=2):
    return [(i, size - 1 - i) for i in range(size)]


def params(semantics, mib=28):
    return pltpu.CompilerParams(dimension_semantics=semantics, vmem_limit_bytes=mib * 1024 * 1024)


def cost(flops, moved):
    return pl.CostEstimate(flops=flops, bytes_accessed=moved, transcendentals=0)


def nt(lhs, rhs):
    return lax.dot_general(lhs, rhs, (((1,), (1,)), ((), ())), preferred_element_type=F32)


def near(position, j):
    if not isinstance(j, int):
        offset = jnp.where(j == 1, 3, jnp.where(j == 2, 1, jnp.where(j == 3, 2, 0)))
    else:
        offset = RELATIVE[j] % 4
    return lax.rem(position + offset, 4)


def norm_kernel(width, values, upstream, gains, *outs):
    pieces, total, acc = outs[:-2], outs[-2], outs[-1]

    @pl.when((pl.program_id(0) == 0) & (pl.program_id(1) == 0))
    def _():
        acc[...] = jnp.zeros_like(acc)

    v = values[0].astype(F32)
    u = upstream[0].astype(F32)
    inverse = lax.rsqrt(jnp.mean(v * v, axis=-1, keepdims=True) + 1e-06)
    n = v * inverse
    acc[...] += jnp.sum((u * n).reshape(-1, 8, u.shape[-1]), axis=0)
    total[...] = jnp.sum(acc[...], axis=0, keepdims=True)
    w = u * gains[...][None, :]
    back = (inverse * (w - n * jnp.mean(w * n, axis=-1, keepdims=True))).astype(BF16)
    for runs, out in zip(PIECES, pieces):
        at = 0
        for z in range(4):
            for start, size in runs:
                out[0, :, at : at + size] = back[:, z * width + start : z * width + start + size]
                at += size


def norm_pieces(projected, out_grad, gains, step=64):
    micro, rows, cols = projected.shape
    block = pl.BlockSpec((1, step, cols), lambda m, i: (m, i, 0))
    return pl.pallas_call(
        functools.partial(norm_kernel, cols // 4),
        grid=(micro, rows // step),
        in_specs=[block, block, pl.BlockSpec((cols,), lambda m, i: (0,))],
        out_specs=[pl.BlockSpec((1, step, 4 * s), lambda m, i: (m, i, 0)) for s in SIZES]
        + [pl.BlockSpec((1, cols), lambda m, i: (0, 0))],
        out_shape=[jax.ShapeDtypeStruct((micro, rows, 4 * s), BF16) for s in SIZES]
        + [jax.ShapeDtypeStruct((1, cols), F32)],
        scratch_shapes=[pltpu.VMEM((8, cols), F32)],
        compiler_params=params(("arbitrary", "arbitrary"), 63),
        cost_estimate=cost(16 * micro * rows * cols, 6 * micro * rows * cols),
        name="norm_back",
    )(projected, out_grad, gains)


def turn_kernel(place, rows, out):
    heads = rows.shape[-1]
    eye = (
        lax.broadcasted_iota(jnp.int32, (heads, heads), 0)
        == lax.broadcasted_iota(jnp.int32, (heads, heads), 1)
    ).astype(BF16)
    taken = [rows[m, near(place[0], j), 0] for j in range(4) for m in range(rows.shape[0])]
    out[0] = nt(eye, jnp.concatenate(taken, axis=0)).astype(BF16)


def turned(attention, place, across):
    micro, rows, heads = attention.shape
    each = rows // 16
    shape = (2, heads, 4 * micro * each)
    return pl.pallas_call(
        turn_kernel,
        grid_spec=pltpu.PrefetchScalarGridSpec(
            num_scalar_prefetch=1,
            grid=(2,),
            in_specs=[
                pl.BlockSpec(
                    (micro, 4, 1, each, heads),
                    lambda i, p: (0, 0, (p[1] ^ across) * 2 + (p[2] ^ i), 0, 0),
                )
            ],
            out_specs=pl.BlockSpec((1,) + shape[1:], lambda i, p: (i, 0, 0)),
        ),
        out_shape=jax.ShapeDtypeStruct(shape, BF16),
        compiler_params=params(("arbitrary",)),
        cost_estimate=cost(4 * heads * heads * shape[2], 8 * heads * shape[2]),
        name="turn",
    )(place, attention.reshape(micro, 4, 4, each, heads))


def data_kernel(plan, *refs):
    acc, refs = refs[-1], list(refs[:-1])
    step = pl.program_id(0)
    sides = []
    for pieces, number in plan:
        parts = []
        for _ in pieces:
            take, refs = refs[:number], refs[number:]
            parts.append(jnp.concatenate([r[...].reshape(-1, r.shape[-1]) for r in take], axis=0))
        sides.append(parts[0] if len(parts) == 1 else jnp.concatenate(parts, axis=1))
    weights, out = refs[:2], refs[2]

    @pl.when(step == 0)
    def _():
        acc[...] = jnp.zeros_like(acc)

    for h, w in enumerate(weights):
        at = 0
        for (pieces, _), lhs in zip(plan, sides):
            start = PIECES[pieces[0]][0][0]
            columns = slice(start, start + lhs.shape[1])
            acc[h, at : at + lhs.shape[0]] += nt(lhs, w[:, columns])
            at += lhs.shape[0]

    @pl.when(step == 3)
    def _():
        out[...] = acc[...].astype(BF16).reshape(out.shape)


def data_grad(plan, weights):
    flat = [a for _, arrays in plan for piece in arrays for a in piece]
    width = weights[0].shape[1] // 4
    rows = sum(sum(math.prod(a.shape[:-1]) for a in arrays[0]) for _, arrays in plan)

    def rows_spec(a):
        size = a.shape[-1] // 4
        if len(a.shape) == 3:
            return pl.BlockSpec(a.shape[:2] + (size,), lambda t: (0, 0, t))
        return pl.BlockSpec((a.shape[0], size), lambda t: (0, t))

    shape = (2, rows // 256, 2, 128, 256)
    flops = sum(
        2 * math.prod(a.shape) * 512 for _, arrays in plan for piece in arrays for a in piece
    )
    return pl.pallas_call(
        functools.partial(data_kernel, [(k, len(a[0])) for k, a in plan]),
        grid=(4,),
        in_specs=[rows_spec(a) for a in flat] + [pl.BlockSpec((256, width), lambda t: (0, t))] * 2,
        out_specs=pl.BlockSpec(shape, lambda t: (0, 0, 0, 0, 0)),
        out_shape=jax.ShapeDtypeStruct(shape, BF16),
        scratch_shapes=[pltpu.VMEM((2, rows, 256), F32)],
        compiler_params=params(("arbitrary",), 63),
        cost_estimate=cost(flops, 16 * 1024 * width),
        name="data_grad",
    )(*flat, *weights)


def weight_sum(pieces, groups):
    sizes = [piece[0].shape[2] // 4 for piece in pieces]
    total = sum(sizes)
    zs = 1 if total % 512 == 0 else 2
    out = pl.BlockSpec((zs, 2, 256, total), lambda i: (i, 0, 0, 0))
    specs = []
    for size in sizes:
        specs += [pl.BlockSpec((2, 128, zs * size), lambda i: (0, 0, i))] * 3
        specs += [pl.BlockSpec((128, zs * size), lambda i: (0, i))] * 2
    heads = [h for group in groups for h in group]
    specs += [pl.BlockSpec((1, 256, 1024), lambda i, n=n: (n, 0, 0)) for _, n in heads]

    def kernel(*refs):
        ins, outs = refs[: -len(groups)], refs[-len(groups) :]
        at = 0
        for k, size in enumerate(sizes):
            rows = jnp.concatenate(
                [r[...].reshape(-1, zs * size) for r in ins[5 * k : 5 * k + 5]], axis=0
            )
            for h, block in enumerate(ins[5 * len(sizes) :]):
                part = jnp.dot(block[0], rows, preferred_element_type=F32).astype(BF16)
                for n in range(zs):
                    outs[h // 2][n, h % 2, :, at : at + size] = part[:, n * size : (n + 1) * size]
            at += size

    return pl.pallas_call(
        kernel,
        grid=(4 // zs,),
        in_specs=specs,
        out_specs=[out] * len(groups),
        out_shape=[jax.ShapeDtypeStruct((4, 2, 256, total), BF16)] * len(groups),
        compiler_params=params(("arbitrary",)),
        cost_estimate=cost(2 * len(heads) * 1024 * 1024 * total, 20 * 1024 * total),
        name="weight_sum",
    )(*[a for piece in pieces for a in piece], *[h for h, _ in heads])


def place_kernel(place, mine, over, mates, out):
    for j in range(4):
        for h, block in enumerate((mine.at[0], mates.at[0], over.at[0], mates.at[1])):
            at = near(place[0], j) * 4 + (place[1] ^ (h // 2)) * 2 + (place[2] ^ (h % 2))
            out[:, pl.ds(at, 1)] = block[j][:, None]


def placed(place, blocks):
    mine, over, mates = blocks
    shape = mine.shape[1:]
    one = pl.BlockSpec((1,) + shape, lambda i, p: (0, 0, 0, 0, 0))
    two = pl.BlockSpec((2,) + shape, lambda i, p: (0, 0, 0, 0, 0))
    return pl.pallas_call(
        place_kernel,
        grid_spec=pltpu.PrefetchScalarGridSpec(
            num_scalar_prefetch=1,
            grid=(1,),
            in_specs=[one, one, two],
            out_specs=pl.BlockSpec((2, 16, 128, 256), lambda i, p: (0, 0, 0, 0)),
        ),
        out_shape=jax.ShapeDtypeStruct((2, 16, 128, 256), BF16),
        compiler_params=params(("arbitrary",)),
        cost_estimate=cost(1000000, 16 * 1024 * 1024 // 2),
        name="place",
    )(place, mine, over, mates)


def moved(value, axis, pairs):
    return lax.ppermute(value, axis, pairs)


def per_device(projected, out_grad, attention, w_out, gains, main_out, main_gains):
    micro, own_rows, cols = projected.shape
    tokens_all = micro * own_rows * lax.axis_size(AXES)
    factor = 1.0 / math.sqrt(tokens_all)
    here, low = lax.axis_index(Z), lax.axis_index(YL)
    place = jnp.stack([lax.axis_index(X), lax.axis_index(YH), lax.axis_index(C)])

    *own, gain = norm_pieces(projected, out_grad, gains)
    left = [moved(p, X, ring(1)) for p in own]
    right = [moved(p, X, ring(-1)) for p in own]
    far = []
    for k in range(len(own)):
        a, b = left[k][0], right[k][1]
        far.append((moved(a, X, ring(1)), moved(b, X, ring(-1))))

    def exchanged(mine, over):
        over = moved(over, YH, swap())
        mates = jnp.stack([mine[1], over[1]])
        return mine, over, moved(mates, C, swap())

    over = turned(attention, place, 1)
    heads = exchanged(turned(attention, place, 0), over)

    over = moved(w_out, (YL, YH), swap(4))
    weights = (w_out, moved(w_out, C, swap()), over, moved(over, C, swap()))

    for axis, bit in ((YH, 1), (YL, 1), (Z, 1), (Z, 2), (C, 1), (X, 1), (X, 2)):
        pairs = [(i, i ^ bit) for i in range(lax.axis_size(axis))]
        gain = gain + moved(gain, axis, pairs)
    new_gains = main_gains + factor * gain[0]

    plan = [
        (tuple(range(len(own))), [(own[k], left[k], right[k]) for k in range(len(own))]),
        (tuple(range(len(own))), far),
    ]
    over = data_grad(plan, weights[2:])
    mine = data_grad(plan, weights[:2])
    grad = placed(place, exchanged(mine, over))

    def reduced(k):
        pieces = [(own[i], left[i], right[i], *far[i]) for i in SUMS[k]]
        mine, over, mates = heads
        keep, send = weight_sum(pieces, [((mine, 0), (over, 0)), ((mates, 0), (mates, 1))])
        other = moved(send, C, swap())

        def block(step):
            at = lax.rem(here + step + 4, 4)
            a = lax.dynamic_index_in_dim(keep, at, 0, keepdims=False).astype(F32)
            return a + lax.dynamic_index_in_dim(other, at, 0, keepdims=False).astype(F32)

        blocks = [block(step).astype(BF16) for step in (1, -1, 2)]
        got = [moved(value, Z, ring(step)) for value, step in zip(blocks, (1, -1, 2))]
        return (block(0) + sum(g.astype(F32) for g in got)).astype(BF16)

    whole = jnp.concatenate([reduced(k) for k in range(len(SUMS))], axis=2)
    first, second = whole[:, :, : cols // 8], whole[:, :, cols // 8 :]
    ours, theirs = jnp.where(low == 0, first, second), jnp.where(low == 0, second, first)
    total = ours[0].astype(F32)
    for value, axes, pairs in ((theirs[0], YL, swap()), (ours[1], YH, swap()), (theirs[1], (YL, YH), swap(4))):
        got = moved(value, axes, pairs)
        total += got.astype(F32)
    new_out = (main_out.T + factor * total.T).T
    return (grad.reshape(attention.shape), new_out, new_gains)


def solution(mesh):
    torus = Mesh(mesh.devices.reshape(4, 2, 4, 2, 2), AXES)

    return jax.shard_map(
        per_device,
        mesh=torus,
        in_specs=(
            P(None, AXES, None),
            P(None, AXES, None),
            P(None, DP, TENSOR),
            P(TENSOR, None),
            P(),
            P(TENSOR, DP),
            P(),
        ),
        out_specs=(P(None, DP, TENSOR), P(TENSOR, DP), P()),
        check_vma=False,
    )
```

```python
import functools
import math

import jax
import jax.numpy as jnp
from jax import lax
from jax.experimental import pallas as pl
from jax.experimental.pallas import tpu as pltpu
from jax.sharding import Mesh
from jax.sharding import PartitionSpec as P

Z, YL, X, YH, C = AXES = ("dp_0", "dp_1", "tensor_0", "tensor_1", "tensor_2")
DP = (Z, YL)
TENSOR = (X, YH, C)
BF16 = jnp.bfloat16
F32 = jnp.float32

PIECES = (((0, 256),), ((256, 512),), ((768, 384),))
SIZES = tuple(sum(size for _, size in runs) for runs in PIECES)
SUMS = ((0,), (1,), (2,))
RELATIVE = (0, -1, 1, 2)


def ring(step, size=4):
    return [(i, (i + step) % size) for i in range(size)]


def swap(size=2):
    return [(i, size - 1 - i) for i in range(size)]


def params(semantics, mib=28):
    return pltpu.CompilerParams(dimension_semantics=semantics, vmem_limit_bytes=mib * 1024 * 1024)


def cost(flops, moved):
    return pl.CostEstimate(flops=flops, bytes_accessed=moved, transcendentals=0)


def nt(lhs, rhs):
    return lax.dot_general(lhs, rhs, (((1,), (1,)), ((), ())), preferred_element_type=F32)


def near(position, j):
    if not isinstance(j, int):
        offset = jnp.where(j == 1, 3, jnp.where(j == 2, 1, jnp.where(j == 3, 2, 0)))
    else:
        offset = RELATIVE[j] % 4
    return lax.rem(position + offset, 4)


def norm_kernel(width, values, upstream, gains, *outs):
    pieces, total, acc = outs[:-2], outs[-2], outs[-1]

    @pl.when((pl.program_id(0) == 0) & (pl.program_id(1) == 0))
    def _():
        acc[...] = jnp.zeros_like(acc)

    v = values[0].astype(F32)
    u = upstream[0].astype(F32)
    inverse = lax.rsqrt(jnp.mean(v * v, axis=-1, keepdims=True) + 1e-06)
    n = v * inverse
    acc[...] += jnp.sum((u * n).reshape(-1, 8, u.shape[-1]), axis=0)
    total[...] = jnp.sum(acc[...], axis=0, keepdims=True)
    w = u * gains[...][None, :]
    back = (inverse * (w - n * jnp.mean(w * n, axis=-1, keepdims=True))).astype(BF16)
    for runs, out in zip(PIECES, pieces):
        at = 0
        for z in range(4):
            for start, size in runs:
                out[0, :, at : at + size] = back[:, z * width + start : z * width + start + size]
                at += size


def norm_pieces(projected, out_grad, gains, step=64):
    micro, rows, cols = projected.shape
    block = pl.BlockSpec((1, step, cols), lambda m, i: (m, i, 0))
    return pl.pallas_call(
        functools.partial(norm_kernel, cols // 4),
        grid=(micro, rows // step),
        in_specs=[block, block, pl.BlockSpec((cols,), lambda m, i: (0,))],
        out_specs=[pl.BlockSpec((1, step, 4 * s), lambda m, i: (m, i, 0)) for s in SIZES]
        + [pl.BlockSpec((1, cols), lambda m, i: (0, 0))],
        out_shape=[jax.ShapeDtypeStruct((micro, rows, 4 * s), BF16) for s in SIZES]
        + [jax.ShapeDtypeStruct((1, cols), F32)],
        scratch_shapes=[pltpu.VMEM((8, cols), F32)],
        compiler_params=params(("arbitrary", "arbitrary"), 63),
        cost_estimate=cost(16 * micro * rows * cols, 6 * micro * rows * cols),
        name="norm_back",
    )(projected, out_grad, gains)


def turn_kernel(place, rows, first, second):
    heads = rows.shape[-1]
    eye = (
        lax.broadcasted_iota(jnp.int32, (heads, heads), 0)
        == lax.broadcasted_iota(jnp.int32, (heads, heads), 1)
    ).astype(BF16)
    taken = [rows[m, near(place[0], j), 0] for j in range(4) for m in range(rows.shape[0])]
    part = nt(eye, jnp.concatenate(taken, axis=0)).astype(BF16)

    @pl.when(pl.program_id(0) == 0)
    def _():
        first[...] = part

    @pl.when(pl.program_id(0) == 1)
    def _():
        second[...] = part


def turned(attention, place, across):
    micro, rows, heads = attention.shape
    each = rows // 16
    shape = (heads, 4 * micro * each)
    return pl.pallas_call(
        turn_kernel,
        grid_spec=pltpu.PrefetchScalarGridSpec(
            num_scalar_prefetch=1,
            grid=(2,),
            in_specs=[
                pl.BlockSpec(
                    (micro, 4, 1, each, heads),
                    lambda i, p: (0, 0, (p[1] ^ across) * 2 + (p[2] ^ i), 0, 0),
                )
            ],
            out_specs=[pl.BlockSpec(shape, lambda i, p: (0, 0))] * 2,
        ),
        out_shape=[jax.ShapeDtypeStruct(shape, BF16)] * 2,
        compiler_params=params(("arbitrary",)),
        cost_estimate=cost(4 * heads * heads * shape[1], 8 * heads * shape[1]),
        name="turn",
    )(place, attention.reshape(micro, 4, 4, each, heads))


def data_kernel(plan, *refs):
    acc, refs = refs[-1], list(refs[:-1])
    step = pl.program_id(0)
    sides = []
    for pieces, number in plan:
        parts = []
        for _ in pieces:
            take, refs = refs[:number], refs[number:]
            parts.append(jnp.concatenate([r[...].reshape(-1, r.shape[-1]) for r in take], axis=0))
        sides.append(parts[0] if len(parts) == 1 else jnp.concatenate(parts, axis=1))
    weights, outs = refs[:2], refs[2:]

    @pl.when(step == 0)
    def _():
        acc[...] = jnp.zeros_like(acc)

    for h, w in enumerate(weights):
        at = 0
        for (pieces, _), lhs in zip(plan, sides):
            start = PIECES[pieces[0]][0][0]
            columns = slice(start, start + lhs.shape[1])
            acc[h, at : at + lhs.shape[0]] += nt(lhs, w[:, columns])
            at += lhs.shape[0]

    @pl.when(step == 3)
    def _():
        for h, out in enumerate(outs):
            out[...] = acc[h].astype(BF16).reshape(out.shape)


def data_grad(plan, weights):
    flat = [a for _, arrays in plan for piece in arrays for a in piece]
    width = weights[0].shape[1] // 4
    rows = sum(sum(math.prod(a.shape[:-1]) for a in arrays[0]) for _, arrays in plan)

    def rows_spec(a):
        size = a.shape[-1] // 4
        if len(a.shape) == 3:
            return pl.BlockSpec(a.shape[:2] + (size,), lambda t: (0, 0, t))
        return pl.BlockSpec((a.shape[0], size), lambda t: (0, t))

    shape = (rows // 256, 2, 128, 256)
    flops = sum(
        2 * math.prod(a.shape) * 512 for _, arrays in plan for piece in arrays for a in piece
    )
    return pl.pallas_call(
        functools.partial(data_kernel, [(k, len(a[0])) for k, a in plan]),
        grid=(4,),
        in_specs=[rows_spec(a) for a in flat] + [pl.BlockSpec((256, width), lambda t: (0, t))] * 2,
        out_specs=[pl.BlockSpec(shape, lambda t: (0, 0, 0, 0))] * 2,
        out_shape=[jax.ShapeDtypeStruct(shape, BF16)] * 2,
        scratch_shapes=[pltpu.VMEM((2, rows, 256), F32)],
        compiler_params=params(("arbitrary",), 63),
        cost_estimate=cost(flops, 16 * 1024 * width),
        name="data_grad",
    )(*flat, *weights)


def weight_sum(pieces, groups):
    sizes = [piece[0].shape[2] // 4 for piece in pieces]
    total = sum(sizes)
    zs = 1 if total % 512 == 0 else 2
    out = pl.BlockSpec((zs, 2, 256, total), lambda i: (i, 0, 0, 0))
    specs = []
    for size in sizes:
        specs += [pl.BlockSpec((2, 128, zs * size), lambda i: (0, 0, i))] * 3
        specs += [pl.BlockSpec((128, zs * size), lambda i: (0, i))] * 2
    heads = [h for group in groups for h in group]
    specs += [pl.BlockSpec((256, 1024), lambda i: (0, 0))] * len(heads)

    def kernel(*refs):
        ins, outs = refs[: -len(groups)], refs[-len(groups) :]
        at = 0
        for k, size in enumerate(sizes):
            rows = jnp.concatenate(
                [r[...].reshape(-1, zs * size) for r in ins[5 * k : 5 * k + 5]], axis=0
            )
            for h, block in enumerate(ins[5 * len(sizes) :]):
                part = jnp.dot(block[...], rows, preferred_element_type=F32).astype(BF16)
                for n in range(zs):
                    outs[h // 2][n, h % 2, :, at : at + size] = part[:, n * size : (n + 1) * size]
            at += size

    return pl.pallas_call(
        kernel,
        grid=(4 // zs,),
        in_specs=specs,
        out_specs=[out] * len(groups),
        out_shape=[jax.ShapeDtypeStruct((4, 2, 256, total), BF16)] * len(groups),
        compiler_params=params(("arbitrary",)),
        cost_estimate=cost(2 * len(heads) * 1024 * 1024 * total, 20 * 1024 * total),
        name="weight_sum",
    )(*[a for piece in pieces for a in piece], *heads)


def place_kernel(place, *refs):
    out = refs[-1]
    for j in range(4):
        for h, block in enumerate(refs[:-1]):
            at = near(place[0], j) * 4 + (place[1] ^ (h // 2)) * 2 + (place[2] ^ (h % 2))
            out[:, pl.ds(at, 1)] = block[j][:, None]


def placed(place, blocks):
    whole = pl.BlockSpec(blocks[0].shape, lambda i, p: (0, 0, 0, 0))
    return pl.pallas_call(
        place_kernel,
        grid_spec=pltpu.PrefetchScalarGridSpec(
            num_scalar_prefetch=1,
            grid=(1,),
            in_specs=[whole] * 4,
            out_specs=pl.BlockSpec((2, 16, 128, 256), lambda i, p: (0, 0, 0, 0)),
        ),
        out_shape=jax.ShapeDtypeStruct((2, 16, 128, 256), BF16),
        compiler_params=params(("arbitrary",)),
        cost_estimate=cost(1000000, 16 * 1024 * 1024 // 2),
        name="place",
    )(place, *blocks)


def moved(value, axis, pairs):
    return lax.ppermute(value, axis, pairs)


def per_device(projected, out_grad, attention, w_out, gains, main_out, main_gains):
    micro, own_rows, cols = projected.shape
    tokens_all = micro * own_rows * lax.axis_size(AXES)
    factor = 1.0 / math.sqrt(tokens_all)
    here, low = lax.axis_index(Z), lax.axis_index(YL)
    place = jnp.stack([lax.axis_index(X), lax.axis_index(YH), lax.axis_index(C)])

    *own, gain = norm_pieces(projected, out_grad, gains)
    left = [moved(p, X, ring(1)) for p in own]
    right = [moved(p, X, ring(-1)) for p in own]
    far = []
    for k in range(len(own)):
        a, b = left[k][0], right[k][1]
        far.append((moved(a, X, ring(1)), moved(b, X, ring(-1))))

    def exchanged(mine, over):
        over, far_mate = [moved(v, YH, swap()) for v in over]
        mate, far_mate = [moved(v, C, swap()) for v in (mine[1], far_mate)]
        return mine[0], mate, over, far_mate

    over = turned(attention, place, 1)
    heads = exchanged(turned(attention, place, 0), over)

    over = moved(w_out, (YL, YH), swap(4))
    weights = (w_out, moved(w_out, C, swap()), over, moved(over, C, swap()))

    for axis, bit in ((YH, 1), (YL, 1), (Z, 1), (Z, 2), (X, 1), (X, 2), (C, 1)):
        pairs = [(i, i ^ bit) for i in range(lax.axis_size(axis))]
        gain = gain + moved(gain, axis, pairs)
    new_gains = main_gains + factor * gain[0]

    plan = [
        (tuple(range(len(own))), [(own[k], left[k], right[k]) for k in range(len(own))]),
        (tuple(range(len(own))), far),
    ]
    over = data_grad(plan, weights[2:])
    mine = data_grad(plan, weights[:2])
    grad = placed(place, exchanged(mine, over))

    def reduced(k):
        pieces = [(own[i], left[i], right[i], *far[i]) for i in SUMS[k]]
        keep, send = weight_sum(pieces, (heads[0::2], heads[1::2]))
        other = moved(send, C, swap())

        def block(step):
            at = lax.rem(here + step + 4, 4)
            a = lax.dynamic_index_in_dim(keep, at, 0, keepdims=False).astype(F32)
            return a + lax.dynamic_index_in_dim(other, at, 0, keepdims=False).astype(F32)

        blocks = [block(step).astype(BF16) for step in (1, -1, 2)]
        got = [moved(value, Z, ring(step)) for value, step in zip(blocks, (1, -1, 2))]
        return (block(0) + sum(g.astype(F32) for g in got)).astype(BF16)

    whole = jnp.concatenate([reduced(k) for k in range(len(SUMS))], axis=2)
    first, second = whole[:, :, : cols // 8], whole[:, :, cols // 8 :]
    ours, theirs = jnp.where(low == 0, first, second), jnp.where(low == 0, second, first)
    total = ours[0].astype(F32)
    for value, axes, pairs in ((ours[1], YH, swap()), (theirs[0], YL, swap()), (theirs[1], (YL, YH), swap(4))):
        got = moved(value, axes, pairs)
        total += got.astype(F32)
    new_out = main_out + factor * total
    return (grad.reshape(attention.shape), new_out, new_gains)


def solution(mesh):
    torus = Mesh(mesh.devices.reshape(4, 2, 4, 2, 2), AXES)

    return jax.shard_map(
        per_device,
        mesh=torus,
        in_specs=(
            P(None, AXES, None),
            P(None, AXES, None),
            P(None, DP, TENSOR),
            P(TENSOR, None),
            P(),
            P(TENSOR, DP),
            P(),
        ),
        out_specs=(P(None, DP, TENSOR), P(TENSOR, DP), P()),
        check_vma=False,
    )
```
